32 devices in a mesh: dp: 4 (over x, y), tp: 8 (over z, core).
Axes of the slice: x: 2, y: 2, z: 4, core: 2. Of those that a mesh axis runs over, the one named last changes fastest.
Arguments:
- x: bfloat16 [256, 5120], P('dp'), parts along dimension 0
- k_cache: bfloat16 [256, 4096, 8, 128], P('dp', None, 'tp'), parts along dimension 0
- v_cache: bfloat16 [256, 4096, 8, 128], P('dp', None, 'tp'), parts along dimension 0
- gain_a: bfloat16 [5120], replicated
- wq: bfloat16 [5120, 4096], P(None, 'tp')
- wo: bfloat16 [4096, 5120], P('tp')
- gain_m: bfloat16 [5120], replicated
- w_gate: bfloat16 [5120, 32768], P(None, 'tp')
- w_up: bfloat16 [5120, 32768], P(None, 'tp')
- w_down: bfloat16 [32768, 5120], P('tp')
Outputs:
- output: bfloat16 [256, 5120], P('dp'), parts along dimension 0
There are 4 independent parts. The reference program is written for one: setup_inputs(seed, part) draws one part's arguments, and reference() takes and returns one part's arrays. A program takes and returns all parts, laid end to end along the dimension named above; an argument that names none is the same for every part.
All inputs are finite; a program needn't handle non-finite values.
Results may differ from the reference program's by a relative error of at most 0.017.
Values are sent between devices in bfloat16 or wider.
A program may use at most 2 GiB of HBM per device.

```python
import jax
import jax.numpy as jnp
from jax import lax

BATCH = 64
CACHE = 4096
D = 5120
HEADS = 32
KV_HEADS = 8
HEAD = 128
FF = 32768
THETA = 10000


def setup_inputs(seed: int = 0, part: int = 0) -> dict:
    kx, kc, kw, kn, kq, ko, km, kg, ku, kd = jax.random.split(jax.random.key(seed), 10)
    kx, kc, kw = (jax.random.fold_in(k, part) for k in (kx, kc, kw))

    def weights(key, rows, columns):
        return jax.random.normal(key, (rows, columns), jnp.float32) * rows**-0.5

    drawn = {
        "x": jax.random.normal(kx, (BATCH, D), jnp.float32),
        "k_cache": 2 * jax.random.normal(kc, (BATCH, CACHE, KV_HEADS, HEAD), jnp.float32),
        "v_cache": 4 * jax.random.normal(kw, (BATCH, CACHE, KV_HEADS, HEAD), jnp.float32),
        "gain_a": 1 + 0.1 * jax.random.normal(kn, (D,), jnp.float32),
        "wq": 2 * weights(kq, D, HEADS * HEAD),
        "wo": weights(ko, HEADS * HEAD, D),
        "gain_m": 1 + 0.1 * jax.random.normal(km, (D,), jnp.float32),
        "w_gate": weights(kg, D, FF),
        "w_up": weights(ku, D, FF),
        "w_down": 2 * weights(kd, FF, D),
    }
    return {k: v.astype(jnp.bfloat16) for k, v in drawn.items()}


def normed(x, gain):
    wide = x.astype(jnp.float32)
    scale = lax.rsqrt(jnp.mean(wide * wide, -1, keepdims=True) + 1e-6)
    return (wide * scale * gain.astype(jnp.float32)).astype(jnp.bfloat16)


def turned(t, place, theta):
    half = t.shape[-1] // 2
    angle = place.astype(jnp.float32)[:, None] * theta ** (-jnp.arange(half, dtype=jnp.float32) / half)
    cos, sin = jnp.cos(angle)[:, None], jnp.sin(angle)[:, None]
    a, b = t[..., :half].astype(jnp.float32), t[..., half:].astype(jnp.float32)
    return jnp.concatenate([a * cos - b * sin, b * cos + a * sin], -1).astype(jnp.bfloat16)


def matmul(a, w):
    return jnp.dot(a, w, preferred_element_type=jnp.float32).astype(jnp.bfloat16)


def einsum(form, a, b):
    return jnp.einsum(form, a.astype(jnp.float32), b.astype(jnp.float32))


def seen_by(a, wq, k_cache, v_cache, head, theta):
    batch, cache, kv_heads = k_cache.shape[:3]
    place = jnp.full((batch,), cache - 1)
    q = turned(matmul(a, wq).reshape(batch, -1, head), place, theta).reshape(batch, kv_heads, -1, head)
    scores = einsum("bgsd,bugd->bgsu", q, k_cache) * head**-0.5
    weights = jax.nn.softmax(scores, -1).astype(jnp.bfloat16)
    return einsum("bgsu,bugd->bgsd", weights, v_cache).astype(jnp.bfloat16).reshape(batch, -1)


def hidden_of(b, w_gate, w_up):
    gate = jnp.dot(b, w_gate, preferred_element_type=jnp.float32)
    up = jnp.dot(b, w_up, preferred_element_type=jnp.float32)
    return (jax.nn.silu(gate) * up).astype(jnp.bfloat16)


def reference(x, k_cache, v_cache, gain_a, wq, wo, gain_m, w_gate, w_up, w_down):
    seen = seen_by(normed(x, gain_a), wq, k_cache, v_cache, HEAD, THETA)
    h = (x.astype(jnp.float32) + jnp.dot(seen, wo, preferred_element_type=jnp.float32)).astype(jnp.bfloat16)
    hidden = hidden_of(normed(h, gain_m), w_gate, w_up)
    return (h.astype(jnp.float32) + jnp.dot(hidden, w_down, preferred_element_type=jnp.float32)).astype(jnp.bfloat16)
```

```python
import functools

import jax
import jax.numpy as jnp
import numpy as np
from jax import lax
from jax.experimental import pallas as pl
from jax.experimental.pallas import tpu as pltpu
from jax.sharding import PartitionSpec as P

HEAD = 128
THETA = 10000
MESH = pl.DeviceIdType.MESH
F32, BF16 = jnp.float32, jnp.bfloat16

CORES = 2
LINE = 4
SEQS = 4
KV_SLOTS = 3
W_SLOTS = 6
WIDE = 256
ROWS = 16


def kernel(
    x_hbm, k_hbm, v_hbm, gain_a_ref, wq_hbm, wo_hbm, gain_m_ref, w_gate_hbm, w_up_hbm, w_down_hbm, turn_ref,
    y_hbm,
    x_ref, normed_ref, h_ref, y_ref, hidden_ref, q_ref, seen_ref, kv_ref, w_ref,
    own1, pair_out1, pair_in1, line_out1, line_in1,
    own2, pair_out2, pair_in2, line_out2, line_in2,
    x_sem, kv_sem, w_sem, wo_sem, y_sem, sum1_sem, sum2_sem,
):
    batch, cache, _ = k_hbm.shape
    d = x_hbm.shape[1]
    heads = wq_hbm.shape[1] // HEAD
    ff = w_gate_hbm.shape[1]
    half_cache = cache // 2
    half_d, part_d = d // CORES, d // (CORES * LINE)
    row_part = batch // LINE
    steps = batch // SEQS
    chunks = batch // ROWS
    per_chunk = ROWS // SEQS
    ups = ff // WIDE
    downs = d // (2 * WIDE)
    q_blocks = heads * HEAD // WIDE
    wo_blocks = half_d // WIDE
    wo_rows = wo_hbm.shape[0]

    me = lax.axis_index("tp")
    core = lax.rem(me, CORES)
    z = me // CORES
    partner = z * CORES + (1 - core)

    def at_z(r):
        return lax.rem(z + r, LINE)

    def peer(r):
        return at_z(r) * CORES + core

    def aligned(i, m):
        return pl.multiple_of(i, m)

    def kv_copies(i, slot):
        rows = pl.ds(aligned(i * SEQS, SEQS), SEQS)
        return [
            pltpu.make_async_copy(hbm.at[rows], kv_ref.at[slot, which], kv_sem.at[slot, which])
            for which, hbm in enumerate((k_hbm, v_hbm))
        ]

    def wq_copies():
        return [
            pltpu.make_async_copy(wq_hbm.at[:, pl.ds(n * WIDE, WIDE)], w_ref.at[0, n, pl.ds(0, d)], w_sem.at[0, n]) for n in range(q_blocks)
        ]

    def wo_copies():
        return [
            pltpu.make_async_copy(
                wo_hbm.at[:, pl.ds((side * wo_blocks + n) * WIDE, WIDE)],
                w_ref.at[W_SLOTS - 1, side, pl.ds(n * wo_rows, wo_rows)],
                wo_sem.at[side, n],
            )
            for side in range(2)
            for n in range(wo_blocks)
        ]

    def up_copies(u, slot):
        columns = pl.ds(aligned(u * WIDE, WIDE), WIDE)
        return [
            pltpu.make_async_copy(hbm.at[:, columns], w_ref.at[slot, side, pl.ds(0, d)], w_sem.at[slot, side])
            for side, hbm in enumerate((w_gate_hbm, w_up_hbm))
        ]

    def down_copies(n, slot):
        return [
            pltpu.make_async_copy(
                w_down_hbm.at[:, pl.ds(aligned((2 * n + side) * WIDE, WIDE), WIDE)],
                w_ref.at[slot, side, pl.ds(0, ff)],
                w_sem.at[slot, side],
            )
            for side in range(2)
        ]

    def start(copies):
        for copy in copies:
            copy.start()

    def wait(copies):
        for copy in copies:
            copy.wait()

    def wait_recv(copies):
        for copy in copies:
            copy.wait_recv()

    def start_weights(u):
        slot = lax.rem(u, W_SLOTS)

        @pl.when(u < ups)
        def _():
            start(up_copies(u, slot))

        @pl.when((u >= ups) & (u < ups + downs))
        def _():
            start(down_copies(u - ups, slot))

    x_copy = pltpu.make_async_copy(x_hbm, x_ref, x_sem)
    x_copy.start()
    start(wq_copies())
    for i in range(KV_SLOTS):
        start(kv_copies(i, i))
    start(wo_copies())

    barrier = pltpu.get_barrier_semaphore()
    for other in [partner] + [peer(r) for r in range(1, LINE)]:
        pl.semaphore_signal(barrier, inc=1, device_id={"tp": other}, device_id_type=MESH)

    part = 512

    def norm_rows(src, rows, gain):
        count = rows.size
        total = jnp.zeros((count, 1), F32)
        for j in range(d // part):
            wide = src[rows, pl.ds(j * part, part)].astype(F32)
            total += jnp.sum(wide * wide, -1, keepdims=True)
        scale = lax.rsqrt(total / d + 1e-6)
        for j in range(d // part):
            columns = pl.ds(j * part, part)
            wide = src[rows, columns].astype(F32)
            normed_ref[rows, columns] = (wide * scale * gain[:, columns].astype(F32)).astype(BF16)

    x_copy.wait()
    for c in range(chunks):
        norm_rows(x_ref, pl.ds(c * ROWS, ROWS), gain_a_ref)
    wait(wq_copies())
    cos, sin = turn_ref[0:1, :], turn_ref[1:2, :]
    q_ref[...] = jnp.zeros_like(q_ref)
    a = normed_ref[...]
    for n in range(q_blocks):
        q = jnp.dot(a, w_ref[0, n, 0:d], preferred_element_type=F32).astype(BF16).astype(F32)
        for j in range(WIDE // HEAD):
            head = n * (WIDE // HEAD) + j
            t = q[:, j * HEAD : (j + 1) * HEAD]
            t = (t * cos + pltpu.roll(t, HEAD // 2, 1) * sin).astype(BF16).astype(F32)
            q_ref[0, pl.ds(head, batch, stride=2 * heads), :] = t
            q_ref[1, pl.ds(heads + head, batch, stride=2 * heads), :] = t

    pl.semaphore_wait(barrier, LINE)

    def remote(src, dst, send, recv, other):
        return pltpu.make_async_remote_copy(
            src_ref=src, dst_ref=dst, send_sem=send, recv_sem=recv, device_id={"tp": other}, device_id_type=MESH
        )

    class Sum:
        def __init__(self, c, sems, pair_out, pair_in, line_out, line_in, part_of, block_of):
            def one(src, dst, place, other):
                return remote(src, dst, sems.at[c, 0, place], sems.at[c, 1, place], other)

            def gathered(place, n, other):
                return one(block_of(place), block_of(place), n, other)

            steps = range(1, LINE)
            self.pair = lambda: [one(pair_out.at[c], pair_in.at[c], 0, partner)]
            self.line = lambda: [one(part_of(line_out, at_z(r)), line_in.at[c, r - 1], r, peer(r)) for r in steps]
            self.gather = lambda: [gathered(z, 3 + r, peer(r)) for r in steps]
            self.own = lambda: [gathered(z, 7, partner)]
            self.passed = lambda: [gathered(at_z(LINE - r), 7 + r, partner) for r in steps]

        def send_pair(self):
            start(self.pair())

        def send_line(self, add_pair):
            wait_recv(self.pair())
            add_pair()
            start(self.line())

        def send_gather(self, add_line):
            wait_recv(self.line())
            add_line()
            start(self.gather() + self.own())

        def pass_on(self):
            for got, copy in zip(self.gather(), self.passed()):
                got.wait_recv()
                copy.start()

        def finish(self):
            wait_recv(self.own() + self.passed())
            for copy in self.pair() + self.line() + self.gather() + self.own() + self.passed():
                copy.wait_send()

    def sum1(c):
        rows = pl.ds(aligned(c * ROWS, ROWS), ROWS)

        def part_of(ref, place):
            return ref.at[c, :, pl.ds(aligned(place * part_d, part_d), part_d)]

        def block_of(place):
            return h_ref.at[rows, pl.ds(aligned(core * half_d + place * part_d, part_d), part_d)]

        return Sum(c, sum1_sem, pair_out1, pair_in1, line_out1, line_in1, part_of, block_of)

    def add_pair1(c):
        def add():
            for j in range(half_d // part):
                columns = pl.ds(j * part, part)
                line_out1[c, :, columns] = (own1[c, :, columns] + pair_in1[c, :, columns].astype(F32)).astype(BF16)

        return add

    def add_line1(c):
        def add():
            rows = pl.ds(aligned(c * ROWS, ROWS), ROWS)
            mine = pl.ds(aligned(z * part_d, part_d), part_d)
            columns = pl.ds(aligned(core * half_d + z * part_d, part_d), part_d)
            total = own1[c, :, mine] + pair_in1[c, :, mine].astype(F32)
            for r in range(LINE - 1):
                total += line_in1[c, r].astype(F32)
            h_ref[rows, columns] = (x_ref[rows, columns].astype(F32) + total).astype(BF16)

        return add

    scaling = HEAD**-0.5

    def attend(i, slot):
        for s in range(SEQS):
            at = pl.ds(aligned((i * SEQS + s) * 2 * heads, 2 * heads), 2 * heads)
            q = jnp.concatenate([q_ref[0, at, :], q_ref[1, at, :]], 1).astype(BF16)
            keys = jnp.concatenate([kv_ref[slot, 0, s, 0:half_cache], kv_ref[slot, 0, s, half_cache:cache]], 1)
            scores = lax.dot_general(q, keys, (((1,), (1,)), ((), ())), preferred_element_type=F32) * scaling
            top = jnp.max(scores, 1, keepdims=True)
            top = jnp.maximum(top, pltpu.roll(top, heads, 0))
            e = jnp.exp(scores - top)
            total = jnp.sum(e, 1, keepdims=True)
            total = total + pltpu.roll(total, heads, 0)
            weights = (e * (1.0 / total)).astype(BF16)
            values = jnp.concatenate([kv_ref[slot, 1, s, 0:half_cache], kv_ref[slot, 1, s, half_cache:cache]], 1)
            both = jnp.dot(weights, values, preferred_element_type=F32)
            seen_ref[at, :] = both[:, 0:HEAD] + pltpu.roll(both[:, HEAD : 2 * HEAD], heads, 0)

    def project(c):
        seen = jnp.concatenate(
            [seen_ref[pl.ds(c * ROWS * 2 * heads + head, ROWS, stride=2 * heads), :] for head in range(heads)], 1
        ).astype(BF16)
        slot = W_SLOTS - 1
        for n in range(wo_blocks):
            rows, columns = pl.ds(n * wo_rows, wo_rows), pl.ds(n * WIDE, WIDE)
            own1[c, :, columns] = jnp.dot(seen, w_ref[slot, core, rows], preferred_element_type=F32)
            pair_out1[c, :, columns] = jnp.dot(seen, w_ref[slot, 1 - core, rows], preferred_element_type=F32).astype(BF16)

    @pl.loop(0, steps)
    def _(i):
        slot = lax.rem(i, KV_SLOTS)
        c = i // per_chunk
        place = lax.rem(i, per_chunk)
        wait(kv_copies(i, slot))
        attend(i, slot)

        @pl.when(i + KV_SLOTS < steps)
        def _():
            start(kv_copies(i + KV_SLOTS, slot))

        @pl.when(i == steps - KV_SLOTS)
        def _():
            start_weights(0)

        @pl.when(i == steps - KV_SLOTS + 1)
        def _():
            start_weights(1)
            start_weights(2)

        @pl.when(i == steps - KV_SLOTS + 2)
        def _():
            for u in range(3, W_SLOTS - 1):
                start_weights(u)

        @pl.when((place == 0) & (i >= per_chunk))
        def _():
            sum1(c - 1).send_line(add_pair1(c - 1))

        @pl.when((place == 0) & (i >= 2 * per_chunk))
        def _():
            sum1(c - 2).pass_on()

        @pl.when((place == per_chunk - 2) & (i >= per_chunk))
        def _():
            sum1(c - 1).send_gather(add_line1(c - 1))

        @pl.when(place == per_chunk - 1)
        def _():
            @pl.when(i == per_chunk - 1)
            def _():
                wait(wo_copies())

            project(c)
            sum1(c).send_pair()

    start_weights(W_SLOTS - 1)
    last = chunks - 1
    sum1(last - 1).pass_on()
    sum1(last).send_line(add_pair1(last))

    @pl.loop(0, last)
    def _(c):
        sum1(c).finish()
        norm_rows(h_ref, pl.ds(aligned(c * ROWS, ROWS), ROWS), gain_m_ref)

    sum1(last).send_gather(add_line1(last))
    sum1(last).pass_on()
    sum1(last).finish()
    norm_rows(h_ref, pl.ds(last * ROWS, ROWS), gain_m_ref)

    @pl.loop(0, ups)
    def _(u):
        slot = lax.rem(u, W_SLOTS)
        wait(up_copies(u, slot))
        b = normed_ref[...]
        gate = jnp.dot(b, w_ref[slot, 0, 0:d], preferred_element_type=F32)
        up = jnp.dot(b, w_ref[slot, 1, 0:d], preferred_element_type=F32)
        hidden_ref[:, pl.ds(aligned(u * WIDE, WIDE), WIDE)] = (gate * (1.0 / (1.0 + jnp.exp(-gate))) * up).astype(BF16)
        start_weights(u + W_SLOTS)

    def sum2(n):
        def part_of(ref, place):
            return ref.at[n, pl.ds(aligned(place * row_part, row_part), row_part)]

        def block_of(place):
            columns = pl.ds(aligned((2 * n + core) * WIDE, WIDE), WIDE)
            return y_ref.at[pl.ds(aligned(place * row_part, row_part), row_part), columns]

        return Sum(n, sum2_sem, pair_out2, pair_in2, line_out2, line_in2, part_of, block_of)

    def add_pair2(n):
        def add():
            line_out2[n] = (own2[n] + pair_in2[n].astype(F32)).astype(BF16)

        return add

    def add_line2(n):
        def add():
            rows = pl.ds(aligned(z * row_part, row_part), row_part)
            columns = pl.ds(aligned((2 * n + core) * WIDE, WIDE), WIDE)
            total = own2[n, rows] + pair_in2[n, rows].astype(F32)
            for r in range(LINE - 1):
                total += line_in2[n, r].astype(F32)
            y_ref[rows, columns] = (h_ref[rows, columns].astype(F32) + total).astype(BF16)

        return add

    lag_line, lag_gather, lag_pass = 1, 4, 7

    @pl.loop(0, downs + lag_pass)
    def _(t):
        @pl.when(t < downs)
        def _():
            slot = lax.rem(ups + t, W_SLOTS)
            wait(down_copies(t, slot))
            hidden = hidden_ref[...]
            own2[t] = jnp.dot(hidden, w_ref[slot, core, 0:ff], preferred_element_type=F32)
            pair_out2[t] = jnp.dot(hidden, w_ref[slot, 1 - core, 0:ff], preferred_element_type=F32).astype(BF16)
            sum2(t).send_pair()
            start_weights(ups + t + W_SLOTS)

        @pl.when((t >= lag_line) & (t < downs + lag_line))
        def _():
            sum2(t - lag_line).send_line(add_pair2(t - lag_line))

        @pl.when((t >= lag_gather) & (t < downs + lag_gather))
        def _():
            sum2(t - lag_gather).send_gather(add_line2(t - lag_gather))

        @pl.when(t >= lag_pass)
        def _():
            sum2(t - lag_pass).pass_on()

    @pl.loop(0, downs)
    def _(n):
        sum2(n).finish()

    y_copy = pltpu.make_async_copy(y_ref, y_hbm, y_sem)
    y_copy.start()
    y_copy.wait()


def solution(mesh):
    def step(x, k_cache, v_cache, gain_a, wq, wo, gain_m, w_gate, w_up, w_down):
        batch, cache = k_cache.shape[:2]
        d, ff = x.shape[1], w_gate.shape[1]
        heads = wq.shape[1] // HEAD
        half_d, part_d, row_part = d // CORES, d // (CORES * LINE), batch // LINE
        chunks, downs = batch // ROWS, d // (2 * WIDE)
        half = HEAD // 2
        angle = (cache - 1) * float(THETA) ** (-np.arange(half) / half)
        cos, sin = np.cos(angle), np.sin(angle)
        turn = np.zeros((8, HEAD), np.float32)
        turn[0], turn[1] = np.concatenate([cos, cos]), np.concatenate([-sin, sin])
        anywhere, vmem = pl.BlockSpec(memory_space=pl.ANY), pl.BlockSpec(memory_space=pltpu.VMEM)
        dma = pltpu.SemaphoreType.DMA
        return pl.pallas_call(
            kernel,
            name="decoder_layer",
            out_shape=jax.ShapeDtypeStruct(x.shape, BF16),
            in_specs=[anywhere, anywhere, anywhere, vmem, anywhere, anywhere, vmem, anywhere, anywhere, anywhere, vmem],
            out_specs=anywhere,
            scratch_shapes=[
                pltpu.VMEM(x.shape, BF16),
                pltpu.VMEM(x.shape, BF16),
                pltpu.VMEM(x.shape, BF16),
                pltpu.VMEM(x.shape, BF16),
                pltpu.VMEM((batch, ff), BF16),
                pltpu.VMEM((2, batch * 2 * heads, HEAD), F32),
                pltpu.VMEM((batch * 2 * heads, HEAD), F32),
                pltpu.VMEM((KV_SLOTS, 2, SEQS, cache, HEAD), BF16),
                pltpu.VMEM((W_SLOTS, 2, max(d, ff), WIDE), BF16),
                pltpu.VMEM((chunks, ROWS, half_d), F32),
                pltpu.VMEM((chunks, ROWS, half_d), BF16),
                pltpu.VMEM((chunks, ROWS, half_d), BF16),
                pltpu.VMEM((chunks, ROWS, half_d), BF16),
                pltpu.VMEM((chunks, LINE - 1, ROWS, part_d), BF16),
                pltpu.VMEM((downs, batch, WIDE), F32),
                pltpu.VMEM((downs, batch, WIDE), BF16),
                pltpu.VMEM((downs, batch, WIDE), BF16),
                pltpu.VMEM((downs, batch, WIDE), BF16),
                pltpu.VMEM((downs, LINE - 1, row_part, WIDE), BF16),
                dma,
                dma((KV_SLOTS, 2)),
                dma((W_SLOTS, 2)),
                dma((2, half_d // WIDE)),
                dma,
                dma((chunks, 2, 11)),
                dma((downs, 2, 11)),
            ],
            compiler_params=pltpu.CompilerParams(collective_id=0, has_side_effects=True, vmem_limit_bytes=67043328),
        )(
            x,
            k_cache.reshape(batch, cache, HEAD),
            v_cache.reshape(batch, cache, HEAD),
            gain_a.reshape(1, d),
            wq,
            wo,
            gain_m.reshape(1, d),
            w_gate,
            w_up,
            w_down,
            jnp.asarray(turn),
        )

    states, cache, columns, rows_of = P("dp", None), P("dp", None, "tp", None), P(None, "tp"), P("tp", None)
    return jax.shard_map(
        step,
        mesh=mesh,
        in_specs=(states, cache, cache, P(None), columns, rows_of, P(None), columns, columns, rows_of),
        out_specs=states,
        check_vma=False,
    )
```

```python
import functools

import jax
import jax.numpy as jnp
import numpy as np
from jax import lax
from jax.experimental import pallas as pl
from jax.experimental.pallas import tpu as pltpu
from jax.sharding import PartitionSpec as P

HEAD = 128
THETA = 10000
MESH = pl.DeviceIdType.MESH
F32, BF16 = jnp.float32, jnp.bfloat16

CORES = 2
LINE = 4
SEQS = 4
KV_CUTS = 1
KV_SLOTS = 3
EARLY = KV_SLOTS
W_SLOTS = 6
WIDE = 256
LAGS = 1, 5, 9, 12
ROWS = 16


def kernel(
    x_hbm, k_hbm, v_hbm, gain_a_ref, wq_hbm, wo_hbm, gain_m_ref, w_gate_hbm, w_up_hbm, w_down_hbm, turn_ref,
    y_ref,
    x_ref, normed_ref, h_ref, hidden_ref, q_ref, seen_ref, kv_ref, w_ref,
    own1, pair_out1, pair_in1, line_in1,
    own2, pair_out2, pair_in2, line_in2,
    x_sem, kv_sem, w_sem, wo_sem, sum1_sem, sum2_sem,
):
    batch, d = x_hbm.shape
    cache = k_hbm.shape[0] // batch
    heads = wq_hbm.shape[1] // HEAD
    ff = w_gate_hbm.shape[1]
    half_cache = cache // 2
    half_d, part_d = d // CORES, d // (CORES * LINE)
    row_part = batch // LINE
    steps = batch // SEQS
    chunks = batch // ROWS
    per_chunk = ROWS // SEQS
    ups = ff // WIDE
    downs = d // (2 * WIDE)
    q_blocks = heads * HEAD // WIDE
    wo_blocks = half_d // WIDE
    wo_rows = wo_hbm.shape[0]

    me = lax.axis_index("tp")
    core = lax.rem(me, CORES)
    z = me // CORES
    partner = z * CORES + (1 - core)

    def at_z(r):
        return lax.rem(z + r, LINE)

    def peer(r):
        return at_z(r) * CORES + core

    def aligned(i, m):
        return pl.multiple_of(i, m)

    def kv_copies(i, slot):
        part = SEQS * cache // KV_CUTS
        return [
            pltpu.make_async_copy(
                hbm.at[pl.ds(aligned((i * KV_CUTS + j) * part, part), part)],
                kv_ref.at[slot, which, pl.ds(j * part, part)],
                kv_sem.at[slot, which, j],
            )
            for j in range(KV_CUTS)
            for which, hbm in enumerate((k_hbm, v_hbm))
        ]

    def early_copies(u):
        slot = lax.rem(u + steps - EARLY, KV_SLOTS)
        return [
            pltpu.make_async_copy(
                hbm.at[:, pl.ds(aligned((2 * u + j) * HEAD, HEAD), HEAD)],
                kv_ref.at[slot, side, pl.ds(j * d, d)],
                kv_sem.at[slot, side, j],
            )
            for side, hbm in enumerate((w_gate_hbm, w_up_hbm))
            for j in range(2)
        ]

    def wq_copies():
        return [
            pltpu.make_async_copy(wq_hbm.at[:, pl.ds(n * WIDE, WIDE)], w_ref.at[0, n, pl.ds(0, d)], w_sem.at[0, n]) for n in range(q_blocks)
        ]

    def wo_copies():
        return [
            pltpu.make_async_copy(
                wo_hbm.at[:, pl.ds((side * wo_blocks + n) * WIDE, WIDE)],
                w_ref.at[W_SLOTS - 1, side, pl.ds(n * wo_rows, wo_rows)],
                wo_sem.at[side, n],
            )
            for side in range(2)
            for n in range(wo_blocks)
        ]

    def up_copies(u, slot):
        columns = pl.ds(aligned(u * WIDE, WIDE), WIDE)
        return [
            pltpu.make_async_copy(hbm.at[:, columns], w_ref.at[slot, side, pl.ds(0, d)], w_sem.at[slot, side])
            for side, hbm in enumerate((w_gate_hbm, w_up_hbm))
        ]

    def down_copies(n, slot):
        return [
            pltpu.make_async_copy(
                w_down_hbm.at[:, pl.ds(aligned((2 * n + side) * WIDE, WIDE), WIDE)],
                w_ref.at[slot, side, pl.ds(0, ff)],
                w_sem.at[slot, side],
            )
            for side in range(2)
        ]

    def start(copies):
        for copy in copies:
            copy.start()

    def wait(copies):
        for copy in copies:
            copy.wait()

    def wait_recv(copies):
        for copy in copies:
            copy.wait_recv()

    def start_weights(u):
        slot = lax.rem(u, W_SLOTS)

        @pl.when(u < ups - EARLY)
        def _():
            start(up_copies(EARLY + u, slot))

        @pl.when((u >= ups - EARLY) & (u < ups - EARLY + downs))
        def _():
            start(down_copies(u - (ups - EARLY), slot))

    x_copy = pltpu.make_async_copy(x_hbm, x_ref, x_sem)
    x_copy.start()
    start(wq_copies())
    start(kv_copies(0, 0))

    barrier = pltpu.get_barrier_semaphore()
    for other in [partner] + [peer(r) for r in range(1, LINE)]:
        pl.semaphore_signal(barrier, inc=1, device_id={"tp": other}, device_id_type=MESH)

    part = 512

    def norm_rows(src, rows, gain):
        count = rows.size
        total = jnp.zeros((count, 1), F32)
        for j in range(d // part):
            wide = src[rows, pl.ds(j * part, part)].astype(F32)
            total += jnp.sum(wide * wide, -1, keepdims=True)
        scale = lax.rsqrt(total / d + 1e-6)
        for j in range(d // part):
            columns = pl.ds(j * part, part)
            wide = src[rows, columns].astype(F32)
            normed_ref[rows, columns] = (wide * scale * gain[columns].astype(F32).reshape(1, part)).astype(BF16)

    x_copy.wait()
    for c in range(chunks):
        norm_rows(x_ref, pl.ds(c * ROWS, ROWS), gain_a_ref)
    for i in range(1, KV_SLOTS):
        start(kv_copies(i, i))
    start(wo_copies())
    wait(wq_copies())
    cos, sin = turn_ref[0:1, :], turn_ref[1:2, :]
    q_ref[...] = jnp.zeros_like(q_ref)
    a = normed_ref[...]
    for n in range(q_blocks):
        q = jnp.dot(a, w_ref[0, n, 0:d], preferred_element_type=F32).astype(BF16).astype(F32)
        for j in range(WIDE // HEAD):
            head = n * (WIDE // HEAD) + j
            t = q[:, j * HEAD : (j + 1) * HEAD]
            t = (t * cos + pltpu.roll(t, HEAD // 2, 1) * sin).astype(BF16).astype(F32)
            q_ref[0, pl.ds(head, batch, stride=2 * heads), :] = t
            q_ref[1, pl.ds(heads + head, batch, stride=2 * heads), :] = t

    pl.semaphore_wait(barrier, LINE)

    def remote(src, dst, send, recv, other):
        return pltpu.make_async_remote_copy(
            src_ref=src, dst_ref=dst, send_sem=send, recv_sem=recv, device_id={"tp": other}, device_id_type=MESH
        )

    class Sum:
        def __init__(self, c, sems, pair_out, pair_in, line_in, part_of, block_of):
            def one(src, dst, place, other):
                return remote(src, dst, sems.at[c, 0, place], sems.at[c, 1, place], other)

            def gathered(place, n, other):
                return one(block_of(place), block_of(place), n, other)

            steps = range(1, LINE)
            self.pair = lambda: [one(pair_out.at[c], pair_in.at[c], 0, partner)]
            self.line = lambda: [one(part_of(pair_in, at_z(r)), line_in.at[c, r - 1], r, peer(r)) for r in steps]
            self.gather = lambda: [gathered(z, 3 + r, peer(r)) for r in steps]
            self.own = lambda: [gathered(z, 7, partner)]
            self.passed = lambda: [gathered(at_z(LINE - r), 7 + r, partner) for r in steps]

        def send_pair(self):
            start(self.pair())

        def send_line(self, add_pair):
            wait_recv(self.pair())
            add_pair()
            start(self.line())

        def send_gather(self, add_line):
            wait_recv(self.line())
            add_line()
            start(self.gather() + self.own())

        def pass_on(self):
            for got, copy in zip(self.gather(), self.passed()):
                got.wait_recv()
                copy.start()

        def finish(self):
            wait_recv(self.own() + self.passed())
            for copy in self.pair() + self.line() + self.gather() + self.own() + self.passed():
                copy.wait_send()

    def sum1(c):
        rows = pl.ds(aligned(c * ROWS, ROWS), ROWS)

        def part_of(ref, place):
            return ref.at[c, :, pl.ds(aligned(place * part_d, part_d), part_d)]

        def block_of(place):
            return h_ref.at[rows, pl.ds(aligned(core * half_d + place * part_d, part_d), part_d)]

        return Sum(c, sum1_sem, pair_out1, pair_in1, line_in1, part_of, block_of)

    def add_pair1(c):
        def add():
            for j in range(half_d // part):
                columns = pl.ds(j * part, part)
                both = own1[c, :, columns] + pair_in1[c, :, columns].astype(F32)
                own1[c, :, columns] = both
                pair_in1[c, :, columns] = both.astype(BF16)

        return add

    def add_line1(c):
        def add():
            rows = pl.ds(aligned(c * ROWS, ROWS), ROWS)
            mine = pl.ds(aligned(z * part_d, part_d), part_d)
            columns = pl.ds(aligned(core * half_d + z * part_d, part_d), part_d)
            total = own1[c, :, mine]
            for r in range(LINE - 1):
                total += line_in1[c, r].astype(F32)
            h_ref[rows, columns] = (x_ref[rows, columns].astype(F32) + total).astype(BF16)

        return add

    def side_by_side(slot, which, at, rows):
        return jnp.concatenate([kv_ref[slot, which, at : at + rows], kv_ref[slot, which, at + rows : at + 2 * rows]], 1)

    scaling = HEAD**-0.5

    def attend(i, slot):
        def rows(s):
            return pl.ds(aligned((i * SEQS + s) * 2 * heads, 2 * heads), 2 * heads)

        def halves(which, s):
            return side_by_side(slot, which, s * cache, half_cache)

        scores, weights = [], []
        for s in range(SEQS):
            q = jnp.concatenate([q_ref[0, rows(s), :], q_ref[1, rows(s), :]], 1).astype(BF16)
            scores.append(lax.dot_general(q, halves(0, s), (((1,), (1,)), ((), ())), preferred_element_type=F32) * scaling)
        for s in range(SEQS):
            top = jnp.max(scores[s], 1, keepdims=True)
            e = jnp.exp(scores[s] - jnp.maximum(top, pltpu.roll(top, heads, 0)))
            total = jnp.sum(e, 1, keepdims=True)
            weights.append((e * (1.0 / (total + pltpu.roll(total, heads, 0)))).astype(BF16))
        for s in range(SEQS):
            both = jnp.dot(weights[s], halves(1, s), preferred_element_type=F32)
            seen_ref[rows(s), :] = both[:, 0:HEAD] + pltpu.roll(both[:, HEAD : 2 * HEAD], heads, 0)

    def project(c):
        seen = jnp.concatenate(
            [seen_ref[pl.ds(c * ROWS * 2 * heads + head, ROWS, stride=2 * heads), :] for head in range(heads)], 1
        ).astype(BF16)
        slot = W_SLOTS - 1
        for n in range(wo_blocks):
            rows, columns = pl.ds(n * wo_rows, wo_rows), pl.ds(n * WIDE, WIDE)
            own1[c, :, columns] = jnp.dot(seen, w_ref[slot, core, rows], preferred_element_type=F32)
            pair_out1[c, :, columns] = jnp.dot(seen, w_ref[slot, 1 - core, rows], preferred_element_type=F32).astype(BF16)

    @pl.loop(0, steps)
    def _(i):
        slot = lax.rem(i, KV_SLOTS)
        c = i // per_chunk
        place = lax.rem(i, per_chunk)
        wait(kv_copies(i, slot))
        attend(i, slot)

        @pl.when(i + KV_SLOTS < steps)
        def _():
            start(kv_copies(i + KV_SLOTS, slot))

        @pl.when(i >= steps - EARLY)
        def _():
            start(early_copies(i - (steps - EARLY)))

        @pl.when(i == steps - 1)
        def _():
            for u in range(W_SLOTS - 1):
                start_weights(u)

        @pl.when((place == 0) & (i >= per_chunk))
        def _():
            sum1(c - 1).send_line(add_pair1(c - 1))

        @pl.when((place == 0) & (i >= 2 * per_chunk))
        def _():
            sum1(c - 2).pass_on()

        @pl.when((place == per_chunk - 2) & (i >= per_chunk))
        def _():
            sum1(c - 1).send_gather(add_line1(c - 1))

        @pl.when(place == per_chunk - 1)
        def _():
            @pl.when(i == per_chunk - 1)
            def _():
                wait(wo_copies())

            project(c)
            sum1(c).send_pair()

    start_weights(W_SLOTS - 1)
    last = chunks - 1
    sum1(last - 1).pass_on()
    sum1(last).send_line(add_pair1(last))

    @pl.loop(0, last)
    def _(c):
        sum1(c).finish()
        norm_rows(h_ref, pl.ds(aligned(c * ROWS, ROWS), ROWS), gain_m_ref)

    sum1(last).send_gather(add_line1(last))
    sum1(last).pass_on()
    sum1(last).finish()
    norm_rows(h_ref, pl.ds(last * ROWS, ROWS), gain_m_ref)

    def gated(u, w_gate, w_up):
        b = normed_ref[...]
        gate = jnp.dot(b, w_gate, preferred_element_type=F32)
        up = jnp.dot(b, w_up, preferred_element_type=F32)
        hidden_ref[:, pl.ds(aligned(u * WIDE, WIDE), WIDE)] = (gate * (1.0 / (1.0 + jnp.exp(-gate))) * up).astype(BF16)

    @pl.loop(0, EARLY)
    def _(u):
        slot = lax.rem(u + steps - EARLY, KV_SLOTS)
        wait(early_copies(u))
        gated(u, side_by_side(slot, 0, 0, d), side_by_side(slot, 1, 0, d))

    @pl.loop(0, ups - EARLY)
    def _(u):
        slot = lax.rem(u, W_SLOTS)
        wait(up_copies(EARLY + u, slot))
        gated(EARLY + u, w_ref[slot, 0, 0:d], w_ref[slot, 1, 0:d])
        start_weights(u + W_SLOTS)

    def sum2(n):
        def part_of(ref, place):
            return ref.at[n, pl.ds(aligned(place * row_part, row_part), row_part)]

        def block_of(place):
            columns = pl.ds(aligned((2 * n + core) * WIDE, WIDE), WIDE)
            return y_ref.at[pl.ds(aligned(place * row_part, row_part), row_part), columns]

        return Sum(n, sum2_sem, pair_out2, pair_in2, line_in2, part_of, block_of)

    def add_pair2(n):
        def add():
            both = own2[n] + pair_in2[n].astype(F32)
            own2[n] = both
            pair_in2[n] = both.astype(BF16)

        return add

    def add_line2(n):
        def add():
            rows = pl.ds(aligned(z * row_part, row_part), row_part)
            columns = pl.ds(aligned((2 * n + core) * WIDE, WIDE), WIDE)
            total = own2[n, rows]
            for r in range(LINE - 1):
                total += line_in2[n, r].astype(F32)
            y_ref[rows, columns] = (h_ref[rows, columns].astype(F32) + total).astype(BF16)

        return add

    lag_line, lag_gather, lag_pass, lag_end = LAGS

    @pl.loop(0, downs + lag_end)
    def _(t):
        @pl.when(t < downs)
        def _():
            slot = lax.rem(ups - EARLY + t, W_SLOTS)
            wait(down_copies(t, slot))
            hidden = hidden_ref[...]
            own2[t] = jnp.dot(hidden, w_ref[slot, core, 0:ff], preferred_element_type=F32)
            pair_out2[t] = jnp.dot(hidden, w_ref[slot, 1 - core, 0:ff], preferred_element_type=F32).astype(BF16)
            sum2(t).send_pair()
            start_weights(ups - EARLY + t + W_SLOTS)

        @pl.when((t >= lag_line) & (t < downs + lag_line))
        def _():
            sum2(t - lag_line).send_line(add_pair2(t - lag_line))

        @pl.when((t >= lag_gather) & (t < downs + lag_gather))
        def _():
            sum2(t - lag_gather).send_gather(add_line2(t - lag_gather))

        @pl.when((t >= lag_pass) & (t < downs + lag_pass))
        def _():
            sum2(t - lag_pass).pass_on()

        @pl.when(t >= lag_end)
        def _():
            sum2(t - lag_end).finish()


def solution(mesh):
    def step(x, k_cache, v_cache, gain_a, wq, wo, gain_m, w_gate, w_up, w_down):
        batch, cache = k_cache.shape[:2]
        d, ff = x.shape[1], w_gate.shape[1]
        heads = wq.shape[1] // HEAD
        half_d, part_d, row_part = d // CORES, d // (CORES * LINE), batch // LINE
        chunks, downs = batch // ROWS, d // (2 * WIDE)
        half = HEAD // 2
        angle = (cache - 1) * float(THETA) ** (-np.arange(half) / half)
        cos, sin = np.cos(angle), np.sin(angle)
        turn = np.zeros((8, HEAD), np.float32)
        turn[0], turn[1] = np.concatenate([cos, cos]), np.concatenate([-sin, sin])
        anywhere, vmem = pl.BlockSpec(memory_space=pl.ANY), pl.BlockSpec(memory_space=pltpu.VMEM)
        dma = pltpu.SemaphoreType.DMA
        return pl.pallas_call(
            kernel,
            name="decoder_layer",
            out_shape=pltpu.VMEM(x.shape, BF16),
            in_specs=[anywhere, anywhere, anywhere, vmem, anywhere, anywhere, vmem, anywhere, anywhere, anywhere, vmem],
            out_specs=vmem,
            scratch_shapes=[
                pltpu.VMEM(x.shape, BF16),
                pltpu.VMEM(x.shape, BF16),
                pltpu.VMEM(x.shape, BF16),
                pltpu.VMEM((batch, ff), BF16),
                pltpu.VMEM((2, batch * 2 * heads, HEAD), F32),
                pltpu.VMEM((batch * 2 * heads, HEAD), F32),
                pltpu.VMEM((KV_SLOTS, 2, SEQS * cache, HEAD), BF16),
                pltpu.VMEM((W_SLOTS, 2, max(d, ff), WIDE), BF16),
                pltpu.VMEM((chunks, ROWS, half_d), F32),
                pltpu.VMEM((chunks, ROWS, half_d), BF16),
                pltpu.VMEM((chunks, ROWS, half_d), BF16),
                pltpu.VMEM((chunks, LINE - 1, ROWS, part_d), BF16),
                pltpu.VMEM((downs, batch, WIDE), F32),
                pltpu.VMEM((downs, batch, WIDE), BF16),
                pltpu.VMEM((downs, batch, WIDE), BF16),
                pltpu.VMEM((downs, LINE - 1, row_part, WIDE), BF16),
                dma,
                dma((KV_SLOTS, 2, max(2, KV_CUTS))),
                dma((W_SLOTS, 2)),
                dma((2, half_d // WIDE)),
                dma((chunks, 2, 11)),
                dma((downs, 2, 11)),
            ],
            compiler_params=pltpu.CompilerParams(collective_id=0, has_side_effects=True, vmem_limit_bytes=66200000),
        )(
            x,
            k_cache.reshape(batch * cache, HEAD),
            v_cache.reshape(batch * cache, HEAD),
            gain_a,
            wq,
            wo,
            gain_m,
            w_gate,
            w_up,
            w_down,
            jnp.asarray(turn),
        )

    states, cache, columns, rows_of = P("dp", None), P("dp", None, "tp", None), P(None, "tp"), P("tp", None)
    return jax.shard_map(
        step,
        mesh=mesh,
        in_specs=(states, cache, cache, P(None), columns, rows_of, P(None), columns, columns, rows_of),
        out_specs=states,
        check_vma=False,
    )
```

```python
import functools

import jax
import jax.numpy as jnp
import numpy as np
from jax import lax
from jax.experimental import pallas as pl
from jax.experimental.pallas import tpu as pltpu
from jax.sharding import PartitionSpec as P

HEAD = 128
THETA = 10000
MESH = pl.DeviceIdType.MESH
F32, BF16 = jnp.float32, jnp.bfloat16

CORES = 2
LINE = 4
SEQS = 4
KV_CUTS = 1
KV_SLOTS = 3
EARLY = KV_SLOTS
W_SLOTS = 6
WIDE = 256
LAGS = 1, 5, 9, 12
ROWS = 16


def kernel(
    x_hbm, k_hbm, v_hbm, gain_a_hbm, wq_hbm, wo_hbm, gain_m_hbm, w_gate_hbm, w_up_hbm, w_down_hbm, turn_hbm,
    y_ref,
    x_ref, gain_a_ref, gain_m_ref, turn_ref, normed_ref, h_ref, hidden_ref, q_ref, seen_ref, kv_ref, w_ref,
    own1, pair_out1, pair_in1, line_in1,
    own2, pair_out2, pair_in2, line_in2,
    x_sem, kv_sem, w_sem, wo_sem, sum1_sem, sum2_sem,
):
    batch, d = x_hbm.shape
    cache = k_hbm.shape[0] // batch
    heads = wq_hbm.shape[1] // HEAD
    ff = w_gate_hbm.shape[1]
    half_cache = cache // 2
    half_d, part_d = d // CORES, d // (CORES * LINE)
    row_part = batch // LINE
    steps = batch // SEQS
    chunks = batch // ROWS
    per_chunk = ROWS // SEQS
    ups = ff // WIDE
    downs = d // (2 * WIDE)
    q_blocks = heads * HEAD // WIDE
    wo_blocks = half_d // WIDE
    wo_rows = wo_hbm.shape[0]

    me = lax.axis_index("tp")
    core = lax.rem(me, CORES)
    z = me // CORES
    partner = z * CORES + (1 - core)

    def at_z(r):
        return lax.rem(z + r, LINE)

    def peer(r):
        return at_z(r) * CORES + core

    def aligned(i, m):
        return pl.multiple_of(i, m)

    def kv_copies(i, slot):
        part = SEQS * cache // KV_CUTS
        return [
            pltpu.make_async_copy(
                hbm.at[pl.ds(aligned((i * KV_CUTS + j) * part, part), part)],
                kv_ref.at[slot, which, pl.ds(j * part, part)],
                kv_sem.at[slot, which, j],
            )
            for j in range(KV_CUTS)
            for which, hbm in enumerate((k_hbm, v_hbm))
        ]

    def early_copies(u):
        slot = lax.rem(u + steps - EARLY, KV_SLOTS)
        return [
            pltpu.make_async_copy(
                hbm.at[:, pl.ds(aligned((2 * u + j) * HEAD, HEAD), HEAD)],
                kv_ref.at[slot, side, pl.ds(j * d, d)],
                kv_sem.at[slot, side, j],
            )
            for side, hbm in enumerate((w_gate_hbm, w_up_hbm))
            for j in range(2)
        ]

    def wq_copies():
        return [
            pltpu.make_async_copy(wq_hbm.at[:, pl.ds(n * WIDE, WIDE)], w_ref.at[0, n, pl.ds(0, d)], w_sem.at[0, n]) for n in range(q_blocks)
        ]

    def wo_copies():
        return [
            pltpu.make_async_copy(
                wo_hbm.at[:, pl.ds((side * wo_blocks + n) * WIDE, WIDE)],
                w_ref.at[W_SLOTS - 1, side, pl.ds(n * wo_rows, wo_rows)],
                wo_sem.at[side, n],
            )
            for side in range(2)
            for n in range(wo_blocks)
        ]

    def up_copies(u, slot):
        columns = pl.ds(aligned(u * WIDE, WIDE), WIDE)
        return [
            pltpu.make_async_copy(hbm.at[:, columns], w_ref.at[slot, side, pl.ds(0, d)], w_sem.at[slot, side])
            for side, hbm in enumerate((w_gate_hbm, w_up_hbm))
        ]

    def down_copies(n, slot):
        return [
            pltpu.make_async_copy(
                w_down_hbm.at[:, pl.ds(aligned((2 * n + side) * WIDE, WIDE), WIDE)],
                w_ref.at[slot, side, pl.ds(0, ff)],
                w_sem.at[slot, side],
            )
            for side in range(2)
        ]

    def start(copies):
        for copy in copies:
            copy.start()

    def wait(copies):
        for copy in copies:
            copy.wait()

    def wait_recv(copies):
        for copy in copies:
            copy.wait_recv()

    def start_weights(u):
        slot = lax.rem(u, W_SLOTS)

        @pl.when(u < ups - EARLY)
        def _():
            start(up_copies(EARLY + u, slot))

        @pl.when((u >= ups - EARLY) & (u < ups - EARLY + downs))
        def _():
            start(down_copies(u - (ups - EARLY), slot))

    small_copies = [
        pltpu.make_async_copy(src, dst, x_sem.at[n])
        for n, (src, dst) in enumerate(
            ((x_hbm, x_ref), (gain_a_hbm, gain_a_ref), (gain_m_hbm, gain_m_ref), (turn_hbm, turn_ref))
        )
    ]
    start(small_copies)
    start(wq_copies())
    start(kv_copies(0, 0))

    barrier = pltpu.get_barrier_semaphore()
    for other in [partner] + [peer(r) for r in range(1, LINE)]:
        pl.semaphore_signal(barrier, inc=1, device_id={"tp": other}, device_id_type=MESH)

    part = 512

    def norm_rows(src, rows, gain):
        count = rows.size
        total = jnp.zeros((count, 1), F32)
        for j in range(d // part):
            wide = src[rows, pl.ds(j * part, part)].astype(F32)
            total += jnp.sum(wide * wide, -1, keepdims=True)
        scale = lax.rsqrt(total / d + 1e-6)
        for j in range(d // part):
            columns = pl.ds(j * part, part)
            wide = src[rows, columns].astype(F32)
            normed_ref[rows, columns] = (wide * scale * gain[columns].astype(F32).reshape(1, part)).astype(BF16)

    wait(small_copies)
    for c in range(chunks):
        norm_rows(x_ref, pl.ds(c * ROWS, ROWS), gain_a_ref)
    for i in range(1, KV_SLOTS):
        start(kv_copies(i, i))
    start(wo_copies())
    wait(wq_copies())
    cos, sin = turn_ref[0:1, :], turn_ref[1:2, :]
    q_ref[...] = jnp.zeros_like(q_ref)
    a = normed_ref[...]
    for n in range(q_blocks):
        q = jnp.dot(a, w_ref[0, n, 0:d], preferred_element_type=F32).astype(BF16).astype(F32)
        for j in range(WIDE // HEAD):
            head = n * (WIDE // HEAD) + j
            t = q[:, j * HEAD : (j + 1) * HEAD]
            t = (t * cos + pltpu.roll(t, HEAD // 2, 1) * sin).astype(BF16).astype(F32)
            q_ref[0, pl.ds(head, batch, stride=2 * heads), :] = t
            q_ref[1, pl.ds(heads + head, batch, stride=2 * heads), :] = t

    pl.semaphore_wait(barrier, LINE)

    def remote(src, dst, send, recv, other):
        return pltpu.make_async_remote_copy(
            src_ref=src, dst_ref=dst, send_sem=send, recv_sem=recv, device_id={"tp": other}, device_id_type=MESH
        )

    class Sum:
        def __init__(self, c, sems, pair_out, pair_in, line_in, part_of, block_of):
            def one(src, dst, place, other):
                return remote(src, dst, sems.at[c, 0, place], sems.at[c, 1, place], other)

            def gathered(place, n, other):
                return one(block_of(place), block_of(place), n, other)

            steps = range(1, LINE)
            self.pair = lambda: [one(pair_out.at[c], pair_in.at[c], 0, partner)]
            self.line = lambda: [one(part_of(pair_in, at_z(r)), line_in.at[c, r - 1], r, peer(r)) for r in steps]
            self.gather = lambda: [gathered(z, 3 + r, peer(r)) for r in steps]
            self.own = lambda: [gathered(z, 7, partner)]
            self.passed = lambda: [gathered(at_z(LINE - r), 7 + r, partner) for r in steps]

        def send_pair(self):
            start(self.pair())

        def send_line(self, add_pair):
            wait_recv(self.pair())
            add_pair()
            start(self.line())

        def send_gather(self, add_line):
            wait_recv(self.line())
            add_line()
            start(self.gather() + self.own())

        def pass_on(self):
            for got, copy in zip(self.gather(), self.passed()):
                got.wait_recv()
                copy.start()

        def finish(self):
            wait_recv(self.own() + self.passed())
            for copy in self.pair() + self.line() + self.gather() + self.own() + self.passed():
                copy.wait_send()

    def sum1(c):
        rows = pl.ds(aligned(c * ROWS, ROWS), ROWS)

        def part_of(ref, place):
            return ref.at[c, :, pl.ds(aligned(place * part_d, part_d), part_d)]

        def block_of(place):
            return h_ref.at[rows, pl.ds(aligned(core * half_d + place * part_d, part_d), part_d)]

        return Sum(c, sum1_sem, pair_out1, pair_in1, line_in1, part_of, block_of)

    def add_pair1(c):
        def add():
            for j in range(half_d // part):
                columns = pl.ds(j * part, part)
                both = own1[c, :, columns] + pair_in1[c, :, columns].astype(F32)
                own1[c, :, columns] = both
                pair_in1[c, :, columns] = both.astype(BF16)

        return add

    def add_line1(c):
        def add():
            rows = pl.ds(aligned(c * ROWS, ROWS), ROWS)
            mine = pl.ds(aligned(z * part_d, part_d), part_d)
            columns = pl.ds(aligned(core * half_d + z * part_d, part_d), part_d)
            total = own1[c, :, mine]
            for r in range(LINE - 1):
                total += line_in1[c, r].astype(F32)
            h_ref[rows, columns] = (x_ref[rows, columns].astype(F32) + total).astype(BF16)

        return add

    def side_by_side(slot, which, at, rows):
        return jnp.concatenate([kv_ref[slot, which, at : at + rows], kv_ref[slot, which, at + rows : at + 2 * rows]], 1)

    scaling = HEAD**-0.5

    def attend(i, slot):
        def rows(s):
            return pl.ds(aligned((i * SEQS + s) * 2 * heads, 2 * heads), 2 * heads)

        def halves(which, s):
            return side_by_side(slot, which, s * cache, half_cache)

        scores, weights = [], []
        for s in range(SEQS):
            q = jnp.concatenate([q_ref[0, rows(s), :], q_ref[1, rows(s), :]], 1).astype(BF16)
            scores.append(lax.dot_general(q, halves(0, s), (((1,), (1,)), ((), ())), preferred_element_type=F32) * scaling)
        for s in range(SEQS):
            top = jnp.max(scores[s], 1, keepdims=True)
            e = jnp.exp(scores[s] - jnp.maximum(top, pltpu.roll(top, heads, 0)))
            total = jnp.sum(e, 1, keepdims=True)
            weights.append((e * (1.0 / (total + pltpu.roll(total, heads, 0)))).astype(BF16))
        for s in range(SEQS):
            both = jnp.dot(weights[s], halves(1, s), preferred_element_type=F32)
            seen_ref[rows(s), :] = both[:, 0:HEAD] + pltpu.roll(both[:, HEAD : 2 * HEAD], heads, 0)

    def project(c):
        seen = jnp.concatenate(
            [seen_ref[pl.ds(c * ROWS * 2 * heads + head, ROWS, stride=2 * heads), :] for head in range(heads)], 1
        ).astype(BF16)
        slot = W_SLOTS - 1
        for n in range(wo_blocks):
            rows, columns = pl.ds(n * wo_rows, wo_rows), pl.ds(n * WIDE, WIDE)
            own1[c, :, columns] = jnp.dot(seen, w_ref[slot, core, rows], preferred_element_type=F32)
            pair_out1[c, :, columns] = jnp.dot(seen, w_ref[slot, 1 - core, rows], preferred_element_type=F32).astype(BF16)

    @pl.loop(0, steps)
    def _(i):
        slot = lax.rem(i, KV_SLOTS)
        c = i // per_chunk
        place = lax.rem(i, per_chunk)
        wait(kv_copies(i, slot))
        attend(i, slot)

        @pl.when(i + KV_SLOTS < steps)
        def _():
            start(kv_copies(i + KV_SLOTS, slot))

        @pl.when(i >= steps - EARLY)
        def _():
            start(early_copies(i - (steps - EARLY)))

        @pl.when(i == steps - 1)
        def _():
            for u in range(W_SLOTS - 1):
                start_weights(u)

        @pl.when((place == 0) & (i >= per_chunk))
        def _():
            sum1(c - 1).send_line(add_pair1(c - 1))

        @pl.when((place == 0) & (i >= 2 * per_chunk))
        def _():
            sum1(c - 2).pass_on()

        @pl.when((place == per_chunk - 2) & (i >= per_chunk))
        def _():
            sum1(c - 1).send_gather(add_line1(c - 1))

        @pl.when(place == per_chunk - 1)
        def _():
            @pl.when(i == per_chunk - 1)
            def _():
                wait(wo_copies())

            project(c)
            sum1(c).send_pair()

    start_weights(W_SLOTS - 1)
    last = chunks - 1
    sum1(last - 1).pass_on()
    sum1(last).send_line(add_pair1(last))

    @pl.loop(0, last)
    def _(c):
        sum1(c).finish()
        norm_rows(h_ref, pl.ds(aligned(c * ROWS, ROWS), ROWS), gain_m_ref)

    sum1(last).send_gather(add_line1(last))
    sum1(last).pass_on()
    sum1(last).finish()
    norm_rows(h_ref, pl.ds(last * ROWS, ROWS), gain_m_ref)

    def gated(u, w_gate, w_up):
        b = normed_ref[...]
        gate = jnp.dot(b, w_gate, preferred_element_type=F32)
        up = jnp.dot(b, w_up, preferred_element_type=F32)
        hidden_ref[:, pl.ds(aligned(u * WIDE, WIDE), WIDE)] = (gate * (1.0 / (1.0 + jnp.exp(-gate))) * up).astype(BF16)

    @pl.loop(0, ups - EARLY)
    def _(u):
        slot = lax.rem(u, W_SLOTS)
        wait(up_copies(EARLY + u, slot))
        gated(EARLY + u, w_ref[slot, 0, 0:d], w_ref[slot, 1, 0:d])
        start_weights(u + W_SLOTS)

    @pl.loop(0, EARLY)
    def _(u):
        slot = lax.rem(u + steps - EARLY, KV_SLOTS)
        wait(early_copies(u))
        gated(u, side_by_side(slot, 0, 0, d), side_by_side(slot, 1, 0, d))

    def sum2(n):
        def part_of(ref, place):
            return ref.at[n, pl.ds(aligned(place * row_part, row_part), row_part)]

        def block_of(place):
            columns = pl.ds(aligned((2 * n + core) * WIDE, WIDE), WIDE)
            return y_ref.at[pl.ds(aligned(place * row_part, row_part), row_part), columns]

        return Sum(n, sum2_sem, pair_out2, pair_in2, line_in2, part_of, block_of)

    def add_pair2(n):
        def add():
            both = own2[n] + pair_in2[n].astype(F32)
            own2[n] = both
            pair_in2[n] = both.astype(BF16)

        return add

    def add_line2(n):
        def add():
            rows = pl.ds(aligned(z * row_part, row_part), row_part)
            columns = pl.ds(aligned((2 * n + core) * WIDE, WIDE), WIDE)
            total = own2[n, rows]
            for r in range(LINE - 1):
                total += line_in2[n, r].astype(F32)
            y_ref[rows, columns] = (h_ref[rows, columns].astype(F32) + total).astype(BF16)

        return add

    lag_line, lag_gather, lag_pass, lag_end = LAGS

    @pl.loop(0, downs + lag_end)
    def _(t):
        @pl.when(t < downs)
        def _():
            slot = lax.rem(ups - EARLY + t, W_SLOTS)
            wait(down_copies(t, slot))
            hidden = hidden_ref[...]
            own2[t] = jnp.dot(hidden, w_ref[slot, core, 0:ff], preferred_element_type=F32)
            pair_out2[t] = jnp.dot(hidden, w_ref[slot, 1 - core, 0:ff], preferred_element_type=F32).astype(BF16)
            sum2(t).send_pair()
            start_weights(ups - EARLY + t + W_SLOTS)

        @pl.when((t >= lag_line) & (t < downs + lag_line))
        def _():
            sum2(t - lag_line).send_line(add_pair2(t - lag_line))

        @pl.when((t >= lag_gather) & (t < downs + lag_gather))
        def _():
            sum2(t - lag_gather).send_gather(add_line2(t - lag_gather))

        @pl.when((t >= lag_pass) & (t < downs + lag_pass))
        def _():
            sum2(t - lag_pass).pass_on()

        @pl.when(t >= lag_end)
        def _():
            sum2(t - lag_end).finish()


def solution(mesh):
    def step(x, k_cache, v_cache, gain_a, wq, wo, gain_m, w_gate, w_up, w_down):
        batch, cache = k_cache.shape[:2]
        d, ff = x.shape[1], w_gate.shape[1]
        heads = wq.shape[1] // HEAD
        half_d, part_d, row_part = d // CORES, d // (CORES * LINE), batch // LINE
        chunks, downs = batch // ROWS, d // (2 * WIDE)
        half = HEAD // 2
        angle = (cache - 1) * float(THETA) ** (-np.arange(half) / half)
        cos, sin = np.cos(angle), np.sin(angle)
        turn = np.zeros((8, HEAD), np.float32)
        turn[0], turn[1] = np.concatenate([cos, cos]), np.concatenate([-sin, sin])
        anywhere, vmem = pl.BlockSpec(memory_space=pl.ANY), pl.BlockSpec(memory_space=pltpu.VMEM)
        dma = pltpu.SemaphoreType.DMA
        return pl.pallas_call(
            kernel,
            name="decoder_layer",
            out_shape=pltpu.VMEM(x.shape, BF16),
            in_specs=[anywhere] * 11,
            out_specs=vmem,
            scratch_shapes=[
                pltpu.VMEM(x.shape, BF16),
                pltpu.VMEM((d,), BF16),
                pltpu.VMEM((d,), BF16),
                pltpu.VMEM(turn.shape, F32),
                pltpu.VMEM(x.shape, BF16),
                pltpu.VMEM(x.shape, BF16),
                pltpu.VMEM((batch, ff), BF16),
                pltpu.VMEM((2, batch * 2 * heads, HEAD), F32),
                pltpu.VMEM((batch * 2 * heads, HEAD), F32),
                pltpu.VMEM((KV_SLOTS, 2, SEQS * cache, HEAD), BF16),
                pltpu.VMEM((W_SLOTS, 2, max(d, ff), WIDE), BF16),
                pltpu.VMEM((chunks, ROWS, half_d), F32),
                pltpu.VMEM((chunks, ROWS, half_d), BF16),
                pltpu.VMEM((chunks, ROWS, half_d), BF16),
                pltpu.VMEM((chunks, LINE - 1, ROWS, part_d), BF16),
                pltpu.VMEM((downs, batch, WIDE), F32),
                pltpu.VMEM((downs, batch, WIDE), BF16),
                pltpu.VMEM((downs, batch, WIDE), BF16),
                pltpu.VMEM((downs, LINE - 1, row_part, WIDE), BF16),
                dma((4,)),
                dma((KV_SLOTS, 2, max(2, KV_CUTS))),
                dma((W_SLOTS, 2)),
                dma((2, half_d // WIDE)),
                dma((chunks, 2, 11)),
                dma((downs, 2, 11)),
            ],
            compiler_params=pltpu.CompilerParams(collective_id=0, has_side_effects=True, vmem_limit_bytes=66200000),
        )(
            x,
            k_cache.reshape(batch * cache, HEAD),
            v_cache.reshape(batch * cache, HEAD),
            gain_a,
            wq,
            wo,
            gain_m,
            w_gate,
            w_up,
            w_down,
            jnp.asarray(turn),
        )

    states, cache, columns, rows_of = P("dp", None), P("dp", None, "tp", None), P(None, "tp"), P("tp", None)
    return jax.shard_map(
        step,
        mesh=mesh,
        in_specs=(states, cache, cache, P(None), columns, rows_of, P(None), columns, columns, rows_of),
        out_specs=states,
        check_vma=False,
    )
```
